32 devices in a mesh: row: 4 (over y, x), col: 8 (over z, core).
Axes of the slice: x: 2, y: 2, z: 4, core: 2. Of those that a mesh axis runs over, the one named last changes fastest.
Arguments:
- grad_out: bfloat16 [512, 8192], P('col', 'row'), may hold values from -6 to 6
- weight: bfloat16 [28672, 8192], P('col', 'row'), may hold values from -0.0625 to 0.0625
Outputs:
- grad_in: bfloat16 [512, 28672], P('row', 'col')
The draws below stay inside these ranges and needn't reach their ends.
All inputs are finite; a program needn't handle non-finite values.
Results may differ from the reference program's by a relative error of at most 0.001.
Values may be sent and summed in bfloat16 or wider, within the bound.
A program may use at most 64 MiB of HBM per device.

```python
import jax
import jax.numpy as jnp
from jax import lax

D = 8192
FF = 28672
TOKENS = 512


def with_spikes(array, key, source, target, parts, factor):
    def block_of(axis_at):
        return (jnp.arange(array.shape[axis_at]) // (array.shape[axis_at] // parts)).reshape((-1,) + (1,) * (array.ndim - 1 - axis_at))

    near = jax.random.permutation(key, parts)[block_of(target)]
    second = (block_of(target) + parts // 2) % parts
    return jnp.where((block_of(source) == near) | (block_of(source) == second), factor * array, array)


def shard_levels(rng, dims, split, low, top_value):
    def one(dim, blocks):
        heights = jax.random.uniform(jax.random.fold_in(jax.random.fold_in(rng, 6), dim), (blocks,), jnp.float32, low / len(split), top_value / len(split))
        return jnp.repeat(jnp.exp(heights), dims[dim] // blocks).reshape((-1,) + (1,) * (len(dims) - dim - 1))

    factor_of = one(*split[0])
    for cut in split[1:]:
        factor_of = factor_of * one(*cut)
    return factor_of


def centred(own_key, dims, spread, reach, cuts=(), dtype=jnp.bfloat16):
    values = jax.random.normal(own_key, dims, jnp.float32) * spread
    if len(cuts) > 0:
        values = shard_levels(own_key, dims, cuts, -0.22, 0.18) * values
    return jnp.clip(values, min=-reach, max=reach).astype(dtype)


def bell_draw_with(stream_key, dims, spread, bound, split, heavy, held_as=jnp.bfloat16):
    array = spread * jax.random.normal(stream_key, dims, jnp.float32)
    if split:
        array = array * shard_levels(stream_key, dims, split, -0.22, 0.18)
    return jnp.clip(with_spikes(array, jax.random.fold_in(stream_key, 3), *heavy), -bound, bound).astype(held_as)


def setup_inputs(seed: int = 0) -> dict:
    key_list = jax.random.split(jax.random.key(seed), 3)
    grad_out = bell_draw_with(key_list[0], (TOKENS, D), 1.0, 6.0, ((0, 8), (1, 4)), (1, 0, 8, 2.0))
    weight = centred(key_list[1], (FF, D), D ** -0.5, 0.0625, ((0, 8), (1, 4)))
    return {"grad_out": grad_out, "weight": weight}


def reference(grad_out, weight):
    blocks = weight.reshape(8, FF // 8, D)

    def one_block(block):
        return jnp.dot(grad_out, block.T, preferred_element_type=jnp.float32).astype(jnp.bfloat16)

    result = lax.map(one_block, blocks)
    return jnp.transpose(result, (1, 0, 2)).reshape(TOKENS, FF)
```

```python
import functools

import jax
import jax.numpy as jnp
from jax import lax
from jax.experimental import pallas as pl
from jax.experimental.pallas import tpu as pltpu
from jax.sharding import PartitionSpec as P

MESH = pl.DeviceIdType.MESH
PHASES = 4
POWER = 13
TOP = 2.0**9.6
LOG2E = 1.4426950408889634


def contract(rows_block, weight):
    return lax.dot_general(
        rows_block, weight, (((1,), (1,)), ((), ())), preferred_element_type=jnp.float32
    )


def local_plain(grad_out, weight):
    partial_value = contract(lax.all_gather(grad_out, "col", axis=0, tiled=True), weight)
    return lax.psum_scatter(partial_value, "row", scatter_dimension=0, tiled=True).astype(
        jnp.bfloat16
    )


def encode(x, factor):
    y = x * factor
    y2 = y * y
    y4 = y2 * y2
    y8 = y4 * y4
    return (y8 * y4 * y).astype(jnp.bfloat16)


def decode(v, step):
    v = v.astype(jnp.float32)
    a = jnp.maximum(jnp.abs(v), 1e-37)
    y = jnp.exp2(jnp.log(a) * (LOG2E / POWER)) * step
    return jnp.where(v < 0, -y, y)


def kernel(
    Z, phases, chunk,
    g_ref, w_hbm, out_ref,
    w_ref, gbuf, acc, send1, send2, recv1, recv2, s_send, s_recv,
    w_sem, ag_send, ag_recv, fw_send, fw_recv, r_send, r_recv, q_send, q_recv,
):
    row = lax.axis_index("row")
    col = lax.axis_index("col")
    z, core = col // 2, col % 2
    rows = g_ref.shape[0] // phases
    ff, depth = w_hbm.shape
    half = ff // 2
    n_chunks = half // chunk
    partner = {"col": col + 1 - 2 * core}
    peers = [None]
    for k in range(1, Z):
        peers.append({"col": ((z + k) % Z) * 2 + core})
    x_row = row + 1 - 2 * (row % 2)
    y_row = (row + 2) % 4
    d_row = 3 - row
    link = [{"row": x_row}, {"row": y_row}]

    w_copies = []
    for i in range(2):
        for j in range(2):
            q = half // 2
            part = pl.ds(i * half + j * q, q)
            copy = pltpu.make_async_copy(w_hbm.at[part], w_ref.at[part], w_sem.at[2 * i + j])
            copy.start()
            w_copies.append(copy)

    barrier = pltpu.get_barrier_semaphore()
    targets = [partner] + peers[1:] + link
    for t in targets:
        pl.semaphore_signal(barrier, inc=1, device_id=t, device_id_type=MESH)
    pl.semaphore_wait(barrier, len(targets))

    def remote(src, dst, ssem, rsem, to):
        return pltpu.make_async_remote_copy(
            src_ref=src, dst_ref=dst, send_sem=ssem, recv_sem=rsem,
            device_id=to, device_id_type=MESH,
        )

    def shard_rows(s):
        return pl.ds(pl.multiple_of(s * rows, rows), rows)

    ag, own_fw, fw = {}, {}, {}
    for p in range(phases):
        src = g_ref.at[pl.ds(p * rows, rows)]
        dst = gbuf.at[p, shard_rows(col)]
        for k in range(1, Z):
            ag[p, k] = remote(src, dst, ag_send.at[p, k], ag_recv.at[p, k], peers[k])
            ag[p, k].start()
        own_fw[p] = remote(src, dst, fw_send.at[p, 0], fw_recv.at[p, 0], partner)
        own_fw[p].start()
    for p in range(phases):
        gbuf[p, shard_rows(col), :] = g_ref[pl.ds(p * rows, rows), :]

    def forward(p):
        for k in range(1, Z):
            ag[p, k].wait_recv()
            s = ((z + Z - k) % Z) * 2 + core
            block = gbuf.at[p, shard_rows(s)]
            fw[p, k] = remote(block, block, fw_send.at[p, k], fw_recv.at[p, k], partner)
            fw[p, k].start()

    def gathered(p):
        own_fw[p].wait_recv()
        for k in range(1, Z):
            fw[p, k].wait_recv()

    def matmul(p, i):
        @pl.loop(0, n_chunks)
        def _(j):
            at = pl.ds(pl.multiple_of(i * half + j * chunk, chunk), chunk)
            acc[p, :, :, at] = contract(gbuf[p], w_ref[at, :]).reshape(4, 2 * rows, chunk)

    def in_half(i, j):
        return pl.ds(pl.multiple_of(i * half + j * chunk, chunk), chunk)

    def local_cols(j):
        return pl.ds(pl.multiple_of(j * chunk, chunk), chunk)

    def put_scale(p, m, top):
        top = jnp.maximum(top, 1e-28)
        s_send[p, m] = jnp.broadcast_to(top * (1.0 / TOP), (8, 128))
        return TOP / top

    first, second, scales = {}, {}, {}

    def send_first(p, i):
        leaf = y_row if i == 0 else x_row
        to = link[1 - i]
        cols = pl.ds(i * half, half)
        top = jnp.maximum(
            jnp.max(jnp.abs(acc[p, d_row, :, cols]), keepdims=True),
            jnp.max(jnp.abs(acc[p, leaf, :, cols]), keepdims=True),
        )
        factor = put_scale(p, i, top)

        @pl.loop(0, n_chunks)
        def _(j):
            send1[p, i, 0, :, local_cols(j)] = encode(acc[p, d_row, :, in_half(i, j)], factor)
            send1[p, i, 1, :, local_cols(j)] = encode(acc[p, leaf, :, in_half(i, j)], factor)

        scales[p, i] = remote(
            s_send.at[p, i], s_recv.at[p, i], q_send.at[p, i], q_recv.at[p, i], to
        )
        scales[p, i].start()
        first[p, i] = remote(
            send1.at[p, i], recv1.at[p, i], r_send.at[p, i], r_recv.at[p, i], to
        )
        first[p, i].start()

    def combine(p, i):
        dest = x_row if i == 0 else y_row
        scales[p, i].wait_recv()
        first[p, i].wait_recv()
        step = s_recv[p, i][:1, :1]

        def add(j, top):
            total = acc[p, dest, :, in_half(i, j)] + decode(
                recv1[p, i, 0, :, local_cols(j)], step
            )
            acc[p, dest, :, in_half(i, j)] = total
            return jnp.maximum(top, jnp.max(jnp.abs(total), axis=0, keepdims=True))

        tops = lax.fori_loop(0, n_chunks, add, jnp.zeros((1, chunk), jnp.float32))
        factor = put_scale(p, 2 + i, jnp.max(tops, keepdims=True))

        @pl.loop(0, n_chunks)
        def _(j):
            send2[p, i, :, local_cols(j)] = encode(acc[p, dest, :, in_half(i, j)], factor)

        to = link[i]
        scales[p, 2 + i] = remote(
            s_send.at[p, 2 + i], s_recv.at[p, 2 + i], q_send.at[p, 2 + i], q_recv.at[p, 2 + i], to
        )
        scales[p, 2 + i].start()
        second[p, i] = remote(
            send2.at[p, i], recv2.at[p, i], r_send.at[p, 2 + i], r_recv.at[p, 2 + i], to
        )
        second[p, i].start()

    def finish(p, i):
        scales[p, 2 + i].wait_recv()
        second[p, i].wait_recv()
        step1 = s_recv[p, i][:1, :1]
        step2 = s_recv[p, 2 + i][:1, :1]
        span = g_ref.shape[0]

        @pl.loop(0, n_chunks)
        def _(j):
            total = (
                acc[p, row, :, in_half(i, j)]
                + decode(recv1[p, i, 1, :, local_cols(j)], step1)
                + decode(recv2[p, i, :, local_cols(j)], step2)
            ).astype(jnp.bfloat16)
            out_ref[pl.ds(p * rows, rows), in_half(i, j)] = total[:rows]
            out_ref[pl.ds(span + p * rows, rows), in_half(i, j)] = total[rows:]

    forward(0)
    for p in range(phases):
        gathered(p)
        for i in range(2):
            if p == 0:
                w_copies[2 * i].wait()
                w_copies[2 * i + 1].wait()
            matmul(p, i)
            send_first(p, i)
        if p + 1 < phases:
            forward(p + 1)
        if p >= 1:
            combine(p - 1, 0)
            combine(p - 1, 1)
        if p >= 2:
            finish(p - 2, 0)
            finish(p - 2, 1)
    last = phases - 1
    for i in range(2):
        combine(last, i)
    if last >= 1:
        for i in range(2):
            finish(last - 1, i)
    for i in range(2):
        finish(last, i)
    for copy in [*ag.values(), *own_fw.values(), *fw.values()]:
        copy.wait_send()
    for copy in [*first.values(), *second.values(), *scales.values()]:
        copy.wait_send()


def solution(mesh):
    n_row, n_col = mesh.shape["row"], mesh.shape["col"]

    def local(grad_out, weight):
        tokens, depth = grad_out.shape
        ff = weight.shape[0]
        phases = PHASES
        rows = tokens // phases
        chunk = 256
        fits = (
            n_row == 4
            and n_col == 2 * n_row
            and rows % 16 == 0
            and ff % (2 * chunk) == 0
            and depth % 128 == 0
        )
        if not fits:
            return local_plain(grad_out, weight)
        Z = n_col // 2
        half = ff // 2
        bf, f32 = jnp.bfloat16, jnp.float32
        dma = pltpu.SemaphoreType.DMA
        return pl.pallas_call(
            functools.partial(kernel, Z, phases, chunk),
            out_shape=jax.ShapeDtypeStruct((2 * tokens, ff), bf),
            in_specs=[
                pl.BlockSpec(memory_space=pltpu.VMEM),
                pl.BlockSpec(memory_space=pl.ANY),
            ],
            out_specs=pl.BlockSpec(memory_space=pltpu.VMEM),
            scratch_shapes=[
                pltpu.VMEM((ff, depth), bf),
                pltpu.VMEM((phases, n_col * rows, depth), bf),
                pltpu.VMEM((phases, 4, 2 * rows, ff), f32),
                pltpu.VMEM((phases, 2, 2, 2 * rows, half), bf),
                pltpu.VMEM((phases, 2, 2 * rows, half), bf),
                pltpu.VMEM((phases, 2, 2, 2 * rows, half), bf),
                pltpu.VMEM((phases, 2, 2 * rows, half), bf),
                pltpu.VMEM((phases, 4, 8, 128), f32),
                pltpu.VMEM((phases, 4, 8, 128), f32),
                dma((4,)),
                dma((phases, Z)),
                dma((phases, Z)),
                dma((phases, Z)),
                dma((phases, Z)),
                dma((phases, 4)),
                dma((phases, 4)),
                dma((phases, 4)),
                dma((phases, 4)),
            ],
            compiler_params=pltpu.CompilerParams(
                collective_id=0, has_side_effects=True, vmem_limit_bytes=56 * 1024 * 1024
            ),
        )(grad_out, weight)

    return jax.shard_map(
        local,
        mesh=mesh,
        in_specs=(P("col", "row"), P("col", "row")),
        out_specs=P("row", "col"),
        check_vma=False,
    )
```

```python
import functools

import jax
import jax.numpy as jnp
from jax import lax
from jax.experimental import pallas as pl
from jax.experimental.pallas import tpu as pltpu
from jax.sharding import PartitionSpec as P

MESH = pl.DeviceIdType.MESH
SPLIT = (1, 1, 1, 1)
VMEM_BYTES = 48 * 1024 * 1024
POWER = 13
TOP = 2.0**9.6
LOG2E = 1.4426950408889634


def contract(rows_block, weight):
    return lax.dot_general(
        rows_block, weight, (((1,), (1,)), ((), ())), preferred_element_type=jnp.float32
    )


def local_plain(grad_out, weight):
    partial_value = contract(lax.all_gather(grad_out, "col", axis=0, tiled=True), weight)
    return lax.psum_scatter(partial_value, "row", scatter_dimension=0, tiled=True).astype(
        jnp.bfloat16
    )


def encode(x, factor):
    y = x * factor
    y2 = y * y
    y4 = y2 * y2
    y8 = y4 * y4
    return (y8 * y4 * y).astype(jnp.bfloat16)


def decode(v, step):
    v = v.astype(jnp.float32)
    a = jnp.maximum(jnp.abs(v), 1e-37)
    y = jnp.exp2(jnp.log(a) * (LOG2E / POWER)) * step
    return jnp.where(v < 0, -y, y)


def kernel(
    Z, split, chunk, wide,
    g_ref, w_hbm, out_ref, w_ref, s_send, s_recv,
    w_sem, ag_send, ag_recv, fw_send, fw_recv, r_send, r_recv, q_send, q_recv,
    *buffers,
):
    phases = len(split)
    gbuf, acc, send1, send2, recv1, recv2 = (
        buffers[n * phases : (n + 1) * phases] for n in range(6)
    )
    start_of = [sum(split[:p]) for p in range(phases)]
    row = lax.axis_index("row")
    col = lax.axis_index("col")
    z, core = col // 2, col % 2
    ff, depth = w_hbm.shape
    half = ff // 2
    n_chunks = half // chunk
    partner = {"col": col + 1 - 2 * core}
    low = jnp.minimum(z, Z - 1 - z)
    mirrored = z >= Z // 2
    others = []
    for i in range(Z - 1):
        t = i + (i >= low).astype(jnp.int32)
        others.append(jnp.where(mirrored, Z - 1 - t, t))
    at_end = low == 0
    near_end = jnp.where(mirrored, Z - 1, 0)
    x_row = row + 1 - 2 * (row % 2)
    y_row = (row + 2) % 4
    d_row = 3 - row
    link = [{"row": x_row}, {"row": y_row}]

    w_copies = []
    for i in range(2):
        for j in range(2):
            q = half // 2
            part = pl.ds(i * half + j * q, q)
            copy = pltpu.make_async_copy(w_hbm.at[part], w_ref.at[part], w_sem.at[2 * i + j])
            copy.start()
            w_copies.append(copy)

    def chip(t):
        return {"col": t * 2 + core}

    barrier = pltpu.get_barrier_semaphore()
    targets = [partner] + [chip(t) for t in others] + link
    for t in targets:
        pl.semaphore_signal(barrier, inc=1, device_id=t, device_id_type=MESH)
    pl.semaphore_wait(barrier, len(targets))

    def remote(src, dst, ssem, rsem, to):
        return pltpu.make_async_remote_copy(
            src_ref=src, dst_ref=dst, send_sem=ssem, recv_sem=rsem,
            device_id=to, device_id_type=MESH,
        )

    def shard_rows(p, s):
        return pl.ds(pl.multiple_of(s * split[p], split[p]), split[p])

    def own_to(p, i):
        return remote(
            g_ref.at[pl.ds(start_of[p], split[p])], gbuf[p].at[shard_rows(p, col)],
            ag_send.at[p, i], ag_recv.at[p, z], chip(others[i]),
        )

    def arrived(p, i):
        block = gbuf[p].at[shard_rows(p, others[i] * 2 + core)]
        return remote(block, block, ag_send.at[p, i], ag_recv.at[p, others[i]], chip(others[i]))

    own_fw, fw = {}, {}
    for p in range(phases):
        own_to(p, 0).start()
        own_to(p, 1).start()

        @pl.when(at_end)
        def _():
            own_to(p, 2).start()

        own_fw[p] = remote(
            g_ref.at[pl.ds(start_of[p], split[p])], gbuf[p].at[shard_rows(p, col)],
            fw_send.at[p, Z - 1], fw_recv.at[p, Z - 1], partner,
        )
        own_fw[p].start()
    for p in range(phases):
        gbuf[p][shard_rows(p, col), :] = g_ref[pl.ds(start_of[p], split[p]), :]

    def relay(p):
        @pl.when(jnp.logical_not(at_end))
        def _():
            arrived(p, 1).wait_recv()
            block = gbuf[p].at[shard_rows(p, others[1] * 2 + core)]
            remote(
                block, block, ag_send.at[p, 2], ag_recv.at[p, others[1]], chip(near_end)
            ).start()

    def forward(p):
        for i in range(Z - 1):
            if i == 1:
                @pl.when(at_end)
                def _():
                    arrived(p, 1).wait_recv()
            else:
                arrived(p, i).wait_recv()
            block = gbuf[p].at[shard_rows(p, others[i] * 2 + core)]
            fw[p, i] = remote(block, block, fw_send.at[p, i], fw_recv.at[p, i], partner)
            fw[p, i].start()

    def gathered(p):
        own_fw[p].wait_recv()
        for i in range(Z - 1):
            fw[p, i].wait_recv()

    def matmul(p, i):
        @pl.loop(0, half // wide)
        def _(j):
            at = pl.ds(pl.multiple_of(i * half + j * wide, wide), wide)
            product = contract(w_ref[at, :], gbuf[p][...])
            acc[p][:, :, at] = product.T.reshape(4, 2 * split[p], wide)

    def in_half(i, j):
        return pl.ds(pl.multiple_of(i * half + j * chunk, chunk), chunk)

    def local_cols(j):
        return pl.ds(pl.multiple_of(j * chunk, chunk), chunk)

    def put_scale(p, m, top):
        top = jnp.maximum(top, 1e-28)
        s_send[p, m] = jnp.broadcast_to(top * (1.0 / TOP), (8, 128))
        return TOP / top

    first, second, scales = {}, {}, {}

    def send_first(p, i):
        leaf = y_row if i == 0 else x_row
        to = link[1 - i]
        cols = pl.ds(i * half, half)
        top = jnp.maximum(
            jnp.max(jnp.abs(acc[p][d_row, :, cols]), keepdims=True),
            jnp.max(jnp.abs(acc[p][leaf, :, cols]), keepdims=True),
        )
        factor = put_scale(p, i, top)

        @pl.loop(0, n_chunks)
        def _(j):
            send1[p][i, 0, :, local_cols(j)] = encode(acc[p][d_row, :, in_half(i, j)], factor)
            send1[p][i, 1, :, local_cols(j)] = encode(acc[p][leaf, :, in_half(i, j)], factor)

        scales[p, i] = remote(
            s_send.at[p, i], s_recv.at[p, i], q_send.at[p, i], q_recv.at[p, i], to
        )
        scales[p, i].start()
        first[p, i] = remote(
            send1[p].at[i], recv1[p].at[i], r_send.at[p, i], r_recv.at[p, i], to
        )
        first[p, i].start()

    def combine(p, i):
        dest = x_row if i == 0 else y_row
        scales[p, i].wait_recv()
        first[p, i].wait_recv()
        step = s_recv[p, i][:1, :1]

        def add(j, top):
            total = acc[p][dest, :, in_half(i, j)] + decode(
                recv1[p][i, 0, :, local_cols(j)], step
            )
            acc[p][dest, :, in_half(i, j)] = total
            return jnp.maximum(top, jnp.max(jnp.abs(total), axis=0, keepdims=True))

        tops = lax.fori_loop(0, n_chunks, add, jnp.zeros((1, chunk), jnp.float32))
        factor = put_scale(p, 2 + i, jnp.max(tops, keepdims=True))

        @pl.loop(0, n_chunks)
        def _(j):
            send2[p][i, :, local_cols(j)] = encode(acc[p][dest, :, in_half(i, j)], factor)

        to = link[i]
        scales[p, 2 + i] = remote(
            s_send.at[p, 2 + i], s_recv.at[p, 2 + i], q_send.at[p, 2 + i], q_recv.at[p, 2 + i], to
        )
        scales[p, 2 + i].start()
        second[p, i] = remote(
            send2[p].at[i], recv2[p].at[i], r_send.at[p, 2 + i], r_recv.at[p, 2 + i], to
        )
        second[p, i].start()

    def finish(p, i):
        scales[p, 2 + i].wait_recv()
        second[p, i].wait_recv()
        step1 = s_recv[p, i][:1, :1]
        step2 = s_recv[p, 2 + i][:1, :1]
        span = g_ref.shape[0]

        @pl.loop(0, n_chunks)
        def _(j):
            total = (
                acc[p][row, :, in_half(i, j)]
                + decode(recv1[p][i, 1, :, local_cols(j)], step1)
                + decode(recv2[p][i, :, local_cols(j)], step2)
            ).astype(jnp.bfloat16)
            out_ref[pl.ds(start_of[p], split[p]), in_half(i, j)] = total[: split[p]]
            out_ref[pl.ds(span + start_of[p], split[p]), in_half(i, j)] = total[split[p] :]

    relay(0)
    forward(0)
    for p in range(phases):
        gathered(p)
        for i in range(2):
            if p == 0:
                w_copies[2 * i].wait()
                w_copies[2 * i + 1].wait()
            matmul(p, i)
            send_first(p, i)
            if p + 1 < phases and i == 0:
                relay(p + 1)
        if p + 1 < phases:
            forward(p + 1)
        if p >= 1:
            combine(p - 1, 0)
            combine(p - 1, 1)
        if p >= 2:
            finish(p - 2, 0)
            finish(p - 2, 1)
    last = phases - 1
    for i in range(2):
        combine(last, i)
    if last >= 1:
        for i in range(2):
            finish(last - 1, i)
    for i in range(2):
        finish(last, i)
    for p in range(phases):
        for i in range(Z - 1):
            own_to(p, i).wait_send()
    for copy in [*own_fw.values(), *fw.values()]:
        copy.wait_send()
    for copy in [*first.values(), *second.values(), *scales.values()]:
        copy.wait_send()


def solution(mesh):
    n_row, n_col = mesh.shape["row"], mesh.shape["col"]

    def local(grad_out, weight):
        tokens, depth = grad_out.shape
        ff = weight.shape[0]
        quarter = tokens // 4
        split = tuple(quarter * n for n in SPLIT)
        chunk = 256
        fits = (
            n_row == 4
            and n_col == 2 * n_row
            and quarter % 16 == 0
            and ff % (2 * chunk) == 0
            and depth % 128 == 0
        )
        if not fits:
            return local_plain(grad_out, weight)
        Z = n_col // 2
        half = ff // 2
        wide = half // 2
        phases = len(split)
        bf, f32 = jnp.bfloat16, jnp.float32
        dma = pltpu.SemaphoreType.DMA
        return pl.pallas_call(
            functools.partial(kernel, Z, split, chunk, wide),
            out_shape=jax.ShapeDtypeStruct((2 * tokens, ff), bf),
            in_specs=[
                pl.BlockSpec(memory_space=pltpu.VMEM),
                pl.BlockSpec(memory_space=pl.ANY),
            ],
            out_specs=pl.BlockSpec(memory_space=pltpu.VMEM),
            scratch_shapes=[
                pltpu.VMEM((ff, depth), bf),
                pltpu.VMEM((phases, 4, 8, 128), f32),
                pltpu.VMEM((phases, 4, 8, 128), f32),
                dma((4,)),
                *[dma((phases, Z))] * 4,
                *[dma((phases, 4))] * 4,
                *[pltpu.VMEM((n_col * n, depth), bf) for n in split],
                *[pltpu.VMEM((4, 2 * n, ff), f32) for n in split],
                *[pltpu.VMEM((2, 2, 2 * n, half), bf) for n in split],
                *[pltpu.VMEM((2, 2 * n, half), bf) for n in split],
                *[pltpu.VMEM((2, 2, 2 * n, half), bf) for n in split],
                *[pltpu.VMEM((2, 2 * n, half), bf) for n in split],
            ],
            compiler_params=pltpu.CompilerParams(
                collective_id=0, has_side_effects=True, vmem_limit_bytes=VMEM_BYTES
            ),
        )(grad_out, weight)

    return jax.shard_map(
        local,
        mesh=mesh,
        in_specs=(P("col", "row"), P("col", "row")),
        out_specs=P("row", "col"),
        check_vma=False,
    )
```

```python
import functools

import jax
import jax.numpy as jnp
from jax import lax
from jax.experimental import pallas as pl
from jax.experimental.pallas import tpu as pltpu
from jax.sharding import PartitionSpec as P

MESH = pl.DeviceIdType.MESH
SPLIT = (1, 1, 1, 1)
PARTS = (1, 1, 1, 1)
VMEM_BYTES = 48 * 1024 * 1024
POWER = 13
TOP = 2.0**9.6
LOG2E = 1.4426950408889634


def contract(rows_block, weight):
    return lax.dot_general(
        rows_block, weight, (((1,), (1,)), ((), ())), preferred_element_type=jnp.float32
    )


def local_plain(grad_out, weight):
    partial_value = contract(lax.all_gather(grad_out, "col", axis=0, tiled=True), weight)
    return lax.psum_scatter(partial_value, "row", scatter_dimension=0, tiled=True).astype(
        jnp.bfloat16
    )


def fold_max(x):
    x = jnp.abs(x)
    tiles = [
        x[a : a + 8, b : b + 128]
        for a in range(0, x.shape[0], 8)
        for b in range(0, x.shape[1], 128)
    ]
    while len(tiles) > 1:
        odd = tiles[-1:] if len(tiles) % 2 else []
        tiles = [jnp.maximum(s, t) for s, t in zip(tiles[::2], tiles[1::2])] + odd
    return tiles[0]


def spread(tile, shape):
    line = jnp.concatenate([tile] * (shape[1] // 128), axis=1)
    return jnp.concatenate([line] * (shape[0] // 8), axis=0)


def encode(x, factor):
    y = x * spread(factor, x.shape)
    y2 = y * y
    y4 = y2 * y2
    y8 = y4 * y4
    return (y8 * y4 * y).astype(jnp.bfloat16)


def decode(v, step):
    v = v.astype(jnp.float32)
    a = jnp.maximum(jnp.abs(v), 1e-37)
    y = jnp.exp2(jnp.log(a) * (LOG2E / POWER)) * spread(step, v.shape)
    return jnp.where(v < 0, -y, y)


def kernel(
    Z, split, parts, chunk, wide,
    g_ref, w_hbm, out_ref, w_ref, s_send, s_recv,
    w_sem, ag_send, ag_recv, fw_send, fw_recv, r_send, r_recv, q_send, q_recv,
    *buffers,
):
    phases = len(split)
    gbuf, acc, send1, send2, recv1, recv2 = (
        buffers[n * phases : (n + 1) * phases] for n in range(6)
    )
    start_of = [sum(split[:p]) for p in range(phases)]
    row = lax.axis_index("row")
    col = lax.axis_index("col")
    z, core = col // 2, col % 2
    ff, depth = w_hbm.shape
    half = ff // 2
    most = max(parts)
    partner = {"col": col + 1 - 2 * core}
    low = jnp.minimum(z, Z - 1 - z)
    mirrored = z >= Z // 2
    others = []
    for i in range(Z - 1):
        t = i + (i >= low).astype(jnp.int32)
        others.append(jnp.where(mirrored, Z - 1 - t, t))
    at_end = low == 0
    near_end = jnp.where(mirrored, Z - 1, 0)
    x_row = row + 1 - 2 * (row % 2)
    y_row = (row + 2) % 4
    d_row = 3 - row
    link = [{"row": x_row}, {"row": y_row}]

    w_copies = []
    for i in range(2):
        for j in range(2):
            q = half // 2
            part = pl.ds(i * half + j * q, q)
            copy = pltpu.make_async_copy(w_hbm.at[part], w_ref.at[part], w_sem.at[2 * i + j])
            copy.start()
            w_copies.append(copy)

    def chip(t):
        return {"col": t * 2 + core}

    barrier = pltpu.get_barrier_semaphore()
    targets = [partner] + [chip(t) for t in others] + link
    for t in targets:
        pl.semaphore_signal(barrier, inc=1, device_id=t, device_id_type=MESH)
    pl.semaphore_wait(barrier, len(targets))

    def remote(src, dst, ssem, rsem, to):
        return pltpu.make_async_remote_copy(
            src_ref=src, dst_ref=dst, send_sem=ssem, recv_sem=rsem,
            device_id=to, device_id_type=MESH,
        )

    def shard_rows(p, s):
        return pl.ds(pl.multiple_of(s * split[p], split[p]), split[p])

    def own_to(p, i):
        return remote(
            g_ref.at[pl.ds(start_of[p], split[p])], gbuf[p].at[shard_rows(p, col)],
            ag_send.at[p, i], ag_recv.at[p, z], chip(others[i]),
        )

    def arrived(p, i):
        block = gbuf[p].at[shard_rows(p, others[i] * 2 + core)]
        return remote(block, block, ag_send.at[p, i], ag_recv.at[p, others[i]], chip(others[i]))

    own_fw, fw = {}, {}

    def issue(p):
        own_to(p, 1).start()
        own_to(p, 0).start()

        @pl.when(at_end)
        def _():
            own_to(p, 2).start()

        own_fw[p] = remote(
            g_ref.at[pl.ds(start_of[p], split[p])], gbuf[p].at[shard_rows(p, col)],
            fw_send.at[p, Z - 1], fw_recv.at[p, Z - 1], partner,
        )
        own_fw[p].start()

    issue(0)
    for p in range(phases):
        gbuf[p][shard_rows(p, col), :] = g_ref[pl.ds(start_of[p], split[p]), :]

    def relay(p):
        @pl.when(jnp.logical_not(at_end))
        def _():
            arrived(p, 1).wait_recv()
            block = gbuf[p].at[shard_rows(p, others[1] * 2 + core)]
            remote(
                block, block, ag_send.at[p, 2], ag_recv.at[p, others[1]], chip(near_end)
            ).start()

    def forward(p):
        for i in range(Z - 1):
            if i == 1:
                @pl.when(at_end)
                def _():
                    arrived(p, 1).wait_recv()
            else:
                arrived(p, i).wait_recv()
            block = gbuf[p].at[shard_rows(p, others[i] * 2 + core)]
            fw[p, i] = remote(block, block, fw_send.at[p, i], fw_recv.at[p, i], partner)
            fw[p, i].start()

    def gathered(p):
        own_fw[p].wait_recv()
        for i in range(Z - 1):
            fw[p, i].wait_recv()

    def width(p):
        return half // parts[p]

    def base(p, i):
        return i % 2 * half + i // 2 * width(p)

    def matmul(p, i):
        @pl.loop(0, width(p) // wide)
        def _(j):
            at = pl.ds(pl.multiple_of(base(p, i) + j * wide, wide), wide)
            product = contract(w_ref[at, :], gbuf[p][...])
            acc[p][:, :, at] = product.T.reshape(4, 2 * split[p], wide)

    def in_half(p, i, j):
        return pl.ds(pl.multiple_of(base(p, i) + j * chunk, chunk), chunk)

    def local_cols(j):
        return pl.ds(pl.multiple_of(j * chunk, chunk), chunk)

    def put_scale(p, m, top):
        top = jnp.maximum(top, 1e-28)
        s_send[p, m] = top * (1.0 / TOP)
        return TOP / top

    first, second, scales = {}, {}, {}

    def send_first(p, i):
        leaf = y_row if i % 2 == 0 else x_row
        to = link[1 - i % 2]

        def largest(j, top):
            cols = in_half(p, i, j)
            return jnp.maximum(
                top,
                jnp.maximum(fold_max(acc[p][d_row, :, cols]), fold_max(acc[p][leaf, :, cols])),
            )

        top = lax.fori_loop(0, width(p) // chunk, largest, jnp.zeros((8, 128), jnp.float32))
        factor = put_scale(p, i, top)

        @pl.loop(0, width(p) // chunk)
        def _(j):
            send1[p][i, 0, :, local_cols(j)] = encode(acc[p][d_row, :, in_half(p, i, j)], factor)
            send1[p][i, 1, :, local_cols(j)] = encode(acc[p][leaf, :, in_half(p, i, j)], factor)

        scales[p, i] = remote(
            s_send.at[p, i], s_recv.at[p, i], q_send.at[p, i], q_recv.at[p, i], to
        )
        scales[p, i].start()
        first[p, i] = remote(
            send1[p].at[i], recv1[p].at[i], r_send.at[p, i], r_recv.at[p, i], to
        )
        first[p, i].start()

    def combine(p, i):
        dest = x_row if i % 2 == 0 else y_row
        scales[p, i].wait_recv()
        first[p, i].wait_recv()
        step = s_recv[p, i]

        def add(j, top):
            total = acc[p][dest, :, in_half(p, i, j)] + decode(
                recv1[p][i, 0, :, local_cols(j)], step
            )
            acc[p][dest, :, in_half(p, i, j)] = total
            return jnp.maximum(top, fold_max(total))

        tops = lax.fori_loop(0, width(p) // chunk, add, jnp.zeros((8, 128), jnp.float32))
        factor = put_scale(p, 2 * most + i, tops)

        @pl.loop(0, width(p) // chunk)
        def _(j):
            send2[p][i, :, local_cols(j)] = encode(acc[p][dest, :, in_half(p, i, j)], factor)

        to = link[i % 2]
        scales[p, 2 * most + i] = remote(
            s_send.at[p, 2 * most + i], s_recv.at[p, 2 * most + i], q_send.at[p, 2 * most + i], q_recv.at[p, 2 * most + i], to
        )
        scales[p, 2 * most + i].start()
        second[p, i] = remote(
            send2[p].at[i], recv2[p].at[i], r_send.at[p, 2 * most + i], r_recv.at[p, 2 * most + i], to
        )
        second[p, i].start()

    def finish(p, i):
        scales[p, 2 * most + i].wait_recv()
        second[p, i].wait_recv()
        step1 = s_recv[p, i]
        step2 = s_recv[p, 2 * most + i]
        span = g_ref.shape[0]

        @pl.loop(0, width(p) // chunk)
        def _(j):
            total = (
                acc[p][row, :, in_half(p, i, j)]
                + decode(recv1[p][i, 1, :, local_cols(j)], step1)
                + decode(recv2[p][i, :, local_cols(j)], step2)
            ).astype(jnp.bfloat16)
            out_ref[pl.ds(start_of[p], split[p]), in_half(p, i, j)] = total[: split[p]]
            out_ref[pl.ds(span + start_of[p], split[p]), in_half(p, i, j)] = total[split[p] :]

    relay(0)
    if phases > 1:
        issue(1)
    forward(0)
    for p in range(phases):
        gathered(p)
        for i in range(2 * parts[p]):
            if p == 0 and i < 2 * parts[0]:
                if i < 2:
                    w_copies[2 * i].wait()
                if i // 2 == parts[0] - 1:
                    w_copies[2 * (i % 2) + 1].wait()
            matmul(p, i)
            send_first(p, i)
            if p + 1 < phases and i == 0:
                relay(p + 1)
                if p + 2 < phases:
                    issue(p + 2)
        if p + 1 < phases:
            forward(p + 1)
        if p >= 1:
            for i in range(2 * parts[p - 1]):
                combine(p - 1, i)
        if p >= 2:
            for i in range(2 * parts[p - 2]):
                finish(p - 2, i)
    last = phases - 1
    for i in range(2 * parts[last]):
        combine(last, i)
    if last >= 1:
        for i in range(2 * parts[last - 1]):
            finish(last - 1, i)
    for i in range(2 * parts[last]):
        finish(last, i)
    for p in range(phases):
        for i in range(Z - 1):
            own_to(p, i).wait_send()
    for copy in [*own_fw.values(), *fw.values()]:
        copy.wait_send()
    for copy in [*first.values(), *second.values(), *scales.values()]:
        copy.wait_send()


def solution(mesh):
    n_row, n_col = mesh.shape["row"], mesh.shape["col"]

    def local(grad_out, weight):
        tokens, depth = grad_out.shape
        ff = weight.shape[0]
        quarter = tokens // 4
        split = tuple(quarter * n for n in SPLIT)
        chunk = ff // 4
        fits = (
            n_row == 4
            and n_col == 2 * n_row
            and quarter % 16 == 0
            and ff % 512 == 0
            and depth % 128 == 0
        )
        if not fits:
            return local_plain(grad_out, weight)
        Z = n_col // 2
        half = ff // 2
        wide = half // 2
        phases = len(split)
        bf, f32 = jnp.bfloat16, jnp.float32
        dma = pltpu.SemaphoreType.DMA
        return pl.pallas_call(
            functools.partial(kernel, Z, split, PARTS, chunk, wide),
            out_shape=jax.ShapeDtypeStruct((2 * tokens, ff), bf),
            in_specs=[
                pl.BlockSpec(memory_space=pltpu.VMEM),
                pl.BlockSpec(memory_space=pl.ANY),
            ],
            out_specs=pl.BlockSpec(memory_space=pltpu.VMEM),
            scratch_shapes=[
                pltpu.VMEM((ff, depth), bf),
                pltpu.VMEM((phases, 4 * max(PARTS), 8, 128), f32),
                pltpu.VMEM((phases, 4 * max(PARTS), 8, 128), f32),
                dma((4,)),
                *[dma((phases, Z))] * 4,
                *[dma((phases, 4 * max(PARTS)))] * 4,
                *[pltpu.VMEM((n_col * n, depth), bf) for n in split],
                *[pltpu.VMEM((4, 2 * n, ff), f32) for n in split],
                *[pltpu.VMEM((2 * k, 2, 2 * n, half // k), bf) for n, k in zip(split, PARTS)],
                *[pltpu.VMEM((2 * k, 2 * n, half // k), bf) for n, k in zip(split, PARTS)],
                *[pltpu.VMEM((2 * k, 2, 2 * n, half // k), bf) for n, k in zip(split, PARTS)],
                *[pltpu.VMEM((2 * k, 2 * n, half // k), bf) for n, k in zip(split, PARTS)],
            ],
            compiler_params=pltpu.CompilerParams(
                collective_id=0, has_side_effects=True, vmem_limit_bytes=VMEM_BYTES
            ),
        )(grad_out, weight)

    return jax.shard_map(
        local,
        mesh=mesh,
        in_specs=(P("col", "row"), P("col", "row")),
        out_specs=P("row", "col"),
        check_vma=False,
    )
```

```python
import functools

import jax
import jax.numpy as jnp
from jax import lax
from jax.experimental import pallas as pl
from jax.experimental.pallas import tpu as pltpu
from jax.sharding import PartitionSpec as P

MESH = pl.DeviceIdType.MESH
SPLIT = (1, 1, 1, 1)
PARTS = (1, 1, 1, 1)
VMEM_BYTES = 48 * 1024 * 1024
POWER = 13
TOP = 2.0**9.6
LOG2E = 1.4426950408889634


def contract(rows_block, weight):
    return lax.dot_general(
        rows_block, weight, (((1,), (1,)), ((), ())), preferred_element_type=jnp.float32
    )


def local_plain(grad_out, weight):
    partial_value = contract(lax.all_gather(grad_out, "col", axis=0, tiled=True), weight)
    return lax.psum_scatter(partial_value, "row", scatter_dimension=0, tiled=True).astype(
        jnp.bfloat16
    )


def fold_max(x):
    x = jnp.abs(x)
    tiles = [
        x[a : a + 8, b : b + 128]
        for a in range(0, x.shape[0], 8)
        for b in range(0, x.shape[1], 128)
    ]
    while len(tiles) > 1:
        odd = tiles[-1:] if len(tiles) % 2 else []
        tiles = [jnp.maximum(s, t) for s, t in zip(tiles[::2], tiles[1::2])] + odd
    return tiles[0]


def spread(tile, shape):
    line = jnp.concatenate([tile] * (shape[1] // 128), axis=1)
    return jnp.concatenate([line] * (shape[0] // 8), axis=0)


def encode(x, factor):
    y = x * spread(factor, x.shape)
    y2 = y * y
    y4 = y2 * y2
    y8 = y4 * y4
    return (y8 * y4 * y).astype(jnp.bfloat16)


def decode(v, step):
    v = v.astype(jnp.float32)
    a = jnp.maximum(jnp.abs(v), 1e-37)
    y = jnp.exp2(jnp.log(a) * (LOG2E / POWER)) * spread(step, v.shape)
    return jnp.where(v < 0, -y, y)


def kernel(
    Z, split, parts, chunk, wide,
    g_ref, w_hbm, out_ref, w_ref,
    w_sem, ag_send, ag_recv, fw_send, fw_recv, r_send, r_recv,
    *buffers,
):
    phases = len(split)
    gbuf, acc, send1, send2, recv1, recv2 = (
        buffers[n * phases : (n + 1) * phases] for n in range(6)
    )
    start_of = [sum(split[:p]) for p in range(phases)]
    row = lax.axis_index("row")
    col = lax.axis_index("col")
    z, core = col // 2, col % 2
    ff, depth = w_hbm.shape
    half = ff // 2
    most = max(parts)
    partner = {"col": col + 1 - 2 * core}
    low = jnp.minimum(z, Z - 1 - z)
    mirrored = z >= Z // 2
    others = []
    for i in range(Z - 1):
        t = i + (i >= low).astype(jnp.int32)
        others.append(jnp.where(mirrored, Z - 1 - t, t))
    at_end = low == 0
    near_end = jnp.where(mirrored, Z - 1, 0)
    x_row = row + 1 - 2 * (row % 2)
    y_row = (row + 2) % 4
    d_row = 3 - row
    link = [{"row": x_row}, {"row": y_row}]

    w_copies = []
    for i in range(2):
        for j in range(2):
            q = half // 2
            part = pl.ds(i * half + j * q, q)
            copy = pltpu.make_async_copy(w_hbm.at[part], w_ref.at[part], w_sem.at[2 * i + j])
            copy.start()
            w_copies.append(copy)

    def chip(t):
        return {"col": t * 2 + core}

    barrier = pltpu.get_barrier_semaphore()
    targets = [partner] + [chip(t) for t in others] + link
    for t in targets:
        pl.semaphore_signal(barrier, inc=1, device_id=t, device_id_type=MESH)
    pl.semaphore_wait(barrier, len(targets))

    def remote(src, dst, ssem, rsem, to):
        return pltpu.make_async_remote_copy(
            src_ref=src, dst_ref=dst, send_sem=ssem, recv_sem=rsem,
            device_id=to, device_id_type=MESH,
        )

    def shard_rows(p, s):
        return pl.ds(pl.multiple_of(s * split[p], split[p]), split[p])

    def own_to(p, i):
        return remote(
            g_ref.at[pl.ds(start_of[p], split[p])], gbuf[p].at[shard_rows(p, col)],
            ag_send.at[p, i], ag_recv.at[p, z], chip(others[i]),
        )

    def arrived(p, i):
        block = gbuf[p].at[shard_rows(p, others[i] * 2 + core)]
        return remote(block, block, ag_send.at[p, i], ag_recv.at[p, others[i]], chip(others[i]))

    own_fw, fw = {}, {}

    def issue(p):
        own_to(p, 1).start()
        own_to(p, 0).start()

        @pl.when(at_end)
        def _():
            own_to(p, 2).start()

        own_fw[p] = remote(
            g_ref.at[pl.ds(start_of[p], split[p])], gbuf[p].at[shard_rows(p, col)],
            fw_send.at[p, Z - 1], fw_recv.at[p, Z - 1], partner,
        )
        own_fw[p].start()

    issue(0)
    for p in range(phases):
        gbuf[p][shard_rows(p, col), :] = g_ref[pl.ds(start_of[p], split[p]), :]

    def relay(p):
        @pl.when(jnp.logical_not(at_end))
        def _():
            arrived(p, 1).wait_recv()
            block = gbuf[p].at[shard_rows(p, others[1] * 2 + core)]
            remote(
                block, block, ag_send.at[p, 2], ag_recv.at[p, others[1]], chip(near_end)
            ).start()

    def forward(p):
        for i in range(Z - 1):
            if i == 1:
                @pl.when(at_end)
                def _():
                    arrived(p, 1).wait_recv()
            else:
                arrived(p, i).wait_recv()
            block = gbuf[p].at[shard_rows(p, others[i] * 2 + core)]
            fw[p, i] = remote(block, block, fw_send.at[p, i], fw_recv.at[p, i], partner)
            fw[p, i].start()

    def gathered(p):
        own_fw[p].wait_recv()
        for i in range(Z - 1):
            fw[p, i].wait_recv()

    def width(p):
        return half // parts[p]

    def base(p, i):
        return i % 2 * half + i // 2 * width(p)

    def matmul(p, i):
        @pl.loop(0, width(p) // wide)
        def _(j):
            at = pl.ds(pl.multiple_of(base(p, i) + j * wide, wide), wide)
            product = contract(w_ref[at, :], gbuf[p][...])
            acc[p][:, :, at] = product.T.reshape(4, 2 * split[p], wide)

    def in_half(p, i, j):
        return pl.ds(pl.multiple_of(base(p, i) + j * chunk, chunk), chunk)

    def step_of(top):
        step = jnp.maximum(top, 1e-28) * (1.0 / TOP)
        return jnp.concatenate([step, step], axis=0).astype(jnp.bfloat16)

    def factor_of(step):
        return 1.0 / step.astype(jnp.float32)[:8]

    def at_group(j, k, high, offset, count):
        start = j * (chunk // 128 * high) + (k * high + offset)
        return pl.ds(pl.multiple_of(start, 16), count)

    def store_coded(ref, i, j, high, offset, value):
        for k in range(chunk // 128):
            rows = at_group(j, k, high, offset, value.shape[0])
            ref[i, rows, :] = value[:, k * 128 : (k + 1) * 128]

    def load_coded(ref, i, j, high, offset, count):
        return jnp.concatenate(
            [ref[i, at_group(j, k, high, offset, count), :] for k in range(chunk // 128)],
            axis=1,
        )

    def step_rows(p, high):
        return pl.ds(width(p) // 128 * high, 16)

    first, second = {}, {}

    def send_first(p, i):
        leaf = y_row if i % 2 == 0 else x_row
        to = link[1 - i % 2]

        def largest(j, top):
            cols = in_half(p, i, j)
            return jnp.maximum(
                top,
                jnp.maximum(fold_max(acc[p][d_row, :, cols]), fold_max(acc[p][leaf, :, cols])),
            )

        top = lax.fori_loop(0, width(p) // chunk, largest, jnp.zeros((8, 128), jnp.float32))
        step = step_of(top)
        factor = factor_of(step)
        n = 2 * split[p]
        send1[p][i, step_rows(p, 2 * n), :] = step

        @pl.loop(0, width(p) // chunk)
        def _(j):
            far = encode(acc[p][d_row, :, in_half(p, i, j)], factor)
            store_coded(send1[p], i, j, 2 * n, 0, far)
            near = encode(acc[p][leaf, :, in_half(p, i, j)], factor)
            store_coded(send1[p], i, j, 2 * n, n, near)

        first[p, i] = remote(
            send1[p].at[i], recv1[p].at[i], r_send.at[p, i], r_recv.at[p, i], to
        )
        first[p, i].start()

    def combine(p, i):
        dest = x_row if i % 2 == 0 else y_row
        first[p, i].wait_recv()
        n = 2 * split[p]
        step = recv1[p][i, step_rows(p, 2 * n), :].astype(jnp.float32)[:8]

        def add(j, top):
            total = acc[p][dest, :, in_half(p, i, j)] + decode(
                load_coded(recv1[p], i, j, 2 * n, 0, n), step
            )
            acc[p][dest, :, in_half(p, i, j)] = total
            return jnp.maximum(top, fold_max(total))

        tops = lax.fori_loop(0, width(p) // chunk, add, jnp.zeros((8, 128), jnp.float32))
        new_step = step_of(tops)
        factor = factor_of(new_step)
        send2[p][i, step_rows(p, n), :] = new_step

        @pl.loop(0, width(p) // chunk)
        def _(j):
            coded = encode(acc[p][dest, :, in_half(p, i, j)], factor)
            store_coded(send2[p], i, j, n, 0, coded)

        to = link[i % 2]
        second[p, i] = remote(
            send2[p].at[i], recv2[p].at[i], r_send.at[p, 2 * most + i], r_recv.at[p, 2 * most + i], to
        )
        second[p, i].start()

    def finish(p, i):
        second[p, i].wait_recv()
        n = 2 * split[p]
        step1 = recv1[p][i, step_rows(p, 2 * n), :].astype(jnp.float32)[:8]
        step2 = recv2[p][i, step_rows(p, n), :].astype(jnp.float32)[:8]
        span = g_ref.shape[0]

        @pl.loop(0, width(p) // chunk)
        def _(j):
            total = (
                acc[p][row, :, in_half(p, i, j)]
                + decode(load_coded(recv1[p], i, j, 2 * n, n, n), step1)
                + decode(load_coded(recv2[p], i, j, n, 0, n), step2)
            ).astype(jnp.bfloat16)
            out_ref[pl.ds(start_of[p], split[p]), in_half(p, i, j)] = total[: split[p]]
            out_ref[pl.ds(span + start_of[p], split[p]), in_half(p, i, j)] = total[split[p] :]

    relay(0)
    if phases > 1:
        issue(1)
    forward(0)
    for p in range(phases):
        gathered(p)
        for i in range(2 * parts[p]):
            if p == 0 and i < 2 * parts[0]:
                if i < 2:
                    w_copies[2 * i].wait()
                if i // 2 == parts[0] - 1:
                    w_copies[2 * (i % 2) + 1].wait()
            matmul(p, i)
            send_first(p, i)
            if p + 1 < phases and i == 0:
                relay(p + 1)
                if p + 2 < phases:
                    issue(p + 2)
        if p + 1 < phases:
            forward(p + 1)
        if p >= 1:
            for i in range(2 * parts[p - 1]):
                combine(p - 1, i)
        if p >= 2:
            for i in range(2 * parts[p - 2]):
                finish(p - 2, i)
    last = phases - 1
    for i in range(2 * parts[last]):
        combine(last, i)
    if last >= 1:
        for i in range(2 * parts[last - 1]):
            finish(last - 1, i)
    for i in range(2 * parts[last]):
        finish(last, i)
    for p in range(phases):
        for i in range(Z - 1):
            own_to(p, i).wait_send()
    for copy in [*own_fw.values(), *fw.values()]:
        copy.wait_send()
    for copy in [*first.values(), *second.values()]:
        copy.wait_send()


def solution(mesh):
    n_row, n_col = mesh.shape["row"], mesh.shape["col"]

    def local(grad_out, weight):
        tokens, depth = grad_out.shape
        ff = weight.shape[0]
        quarter = tokens // 4
        split = tuple(quarter * n for n in SPLIT)
        chunk = ff // 4
        fits = (
            n_row == 4
            and n_col == 2 * n_row
            and quarter % 16 == 0
            and ff % 512 == 0
            and depth % 128 == 0
        )
        if not fits:
            return local_plain(grad_out, weight)
        Z = n_col // 2
        half = ff // 2
        wide = half // 2
        phases = len(split)
        bf, f32 = jnp.bfloat16, jnp.float32
        dma = pltpu.SemaphoreType.DMA
        return pl.pallas_call(
            functools.partial(kernel, Z, split, PARTS, chunk, wide),
            out_shape=jax.ShapeDtypeStruct((2 * tokens, ff), bf),
            in_specs=[
                pl.BlockSpec(memory_space=pltpu.VMEM),
                pl.BlockSpec(memory_space=pl.ANY),
            ],
            out_specs=pl.BlockSpec(memory_space=pltpu.VMEM),
            scratch_shapes=[
                pltpu.VMEM((ff, depth), bf),
                dma((4,)),
                *[dma((phases, Z))] * 4,
                *[dma((phases, 4 * max(PARTS)))] * 2,
                *[pltpu.VMEM((n_col * n, depth), bf) for n in split],
                *[pltpu.VMEM((4, 2 * n, ff), f32) for n in split],
                *[pltpu.VMEM((2 * k, half // k // 128 * 4 * n + 16, 128), bf) for n, k in zip(split, PARTS)],
                *[pltpu.VMEM((2 * k, half // k // 128 * 2 * n + 16, 128), bf) for n, k in zip(split, PARTS)],
                *[pltpu.VMEM((2 * k, half // k // 128 * 4 * n + 16, 128), bf) for n, k in zip(split, PARTS)],
                *[pltpu.VMEM((2 * k, half // k // 128 * 2 * n + 16, 128), bf) for n, k in zip(split, PARTS)],
            ],
            compiler_params=pltpu.CompilerParams(
                collective_id=0, has_side_effects=True, vmem_limit_bytes=VMEM_BYTES
            ),
        )(grad_out, weight)

    return jax.shard_map(
        local,
        mesh=mesh,
        in_specs=(P("col", "row"), P("col", "row")),
        out_specs=P("row", "col"),
        check_vma=False,
    )
```
